32 devices in a mesh: samples: 4 (over y, x), features: 4 (over z), rhs: 2 (over core).
Axes of the slice: x: 2, y: 2, z: 4, core: 2. Of those that a mesh axis runs over, the one named last changes fastest.
Arguments:
- design: bfloat16 [32768, 32768], P(('samples', 'rhs'), 'features'), may hold values from -0.03125 to 0.03125
- right_side: float32 [32768, 64], P('features', 'rhs'), may hold values from -6 to 6
- factor: bfloat16 [32768, 768], P('features', 'rhs'), may hold values from -0.03125 to 0.03125
- nystrom_values: float32 [768], replicated, may hold values from 0.5 to 3
Outputs:
- solution: float32 [32768, 64], P('features', 'rhs')
- residual: float32 [32768, 64], P('features', 'rhs')
The draws below stay inside these ranges and needn't reach their ends.
All inputs are finite; a program needn't handle non-finite values.
Results may differ from the reference program's by a relative error of at most 0.0181.
Values may be sent and summed in bfloat16 or wider, within the bound.
No kernel may reach another device: no remote copies, remote signals or barrier semaphores. Data moves between devices by JAX's collectives and lax.ppermute only.
A program may use at most 192 MiB of HBM per device.

```python
import math
import jax
import jax.numpy as jnp
from jax import lax

F = 32768
K = 64
R = 768
ITERS = 3
NS = 32768


def block_levels(key, shape, cuts, low, top_value):
    level, own = 1.0, jax.random.fold_in(key, 6)
    for dim, shards_of in cuts:
        steps = jnp.exp(jax.random.uniform(jax.random.fold_in(own, dim), (shards_of,), jnp.float32, low / len(cuts), top_value / len(cuts)))
        level = level * jnp.repeat(steps, shape[dim] // shards_of).reshape([-1 if axis == dim else 1 for axis in range(len(shape))])
    return level


def scatter_about(rng, extent, deviation, most, pieces=(), held_as=jnp.bfloat16):
    factor_of = block_levels(rng, extent, pieces, -0.22, 0.18) if pieces else 1.0
    array = jax.random.normal(rng, extent, jnp.float32) * deviation * factor_of
    return jnp.minimum(jnp.maximum(array, -most), most).astype(held_as)


def setup_inputs(seed: int = 0) -> dict:
    splits = jax.random.split(jax.random.key(seed), 5)
    design = scatter_about(splits[0], (NS, F), NS ** -0.5, 0.03125, ((0, 8), (1, 4)))
    right_side = scatter_about(splits[1], (F, K), 1.0, 6.0, ((0, 4), (1, 2)), jnp.float32)
    factor = scatter_about(splits[2], (F, R), F ** -0.5, 0.03125, ((0, 4), (1, 2)))
    nystrom_values = jnp.clip(jnp.exp(jax.random.uniform(splits[3], (R,), jnp.float32, math.log(0.5), math.log(3.0))), 0.5, 3.0)
    return {"design": design, "right_side": right_side, "factor": factor, "nystrom_values": nystrom_values}


ridge_weight = 1.0

def inner_prod(left, right):
    return lax.dot_general(left.astype(jnp.float32), right.astype(jnp.float32), (((0,), (0,)), ((), ())), precision=lax.Precision.HIGHEST, preferred_element_type=jnp.float32)

def apply_operator(design, direction):
    narrow = direction.astype(jnp.bfloat16)
    images = jnp.dot(design.astype(jnp.float32), narrow.astype(jnp.float32), preferred_element_type=jnp.float32).astype(jnp.bfloat16)
    summed = lax.dot_general(design.astype(jnp.float32), images.astype(jnp.float32), (((0,), (0,)), ((), ())), preferred_element_type=jnp.float32)
    return summed + ridge_weight * direction

def reference(design, right_side, factor, nystrom_values):
    shrink = (1.0 + jnp.min(nystrom_values)) / (1.0 + nystrom_values) - 1.0
    factor_wide = factor.astype(jnp.float32)

    def precondition(values):
        projected = inner_prod(factor_wide, values)
        return values + jnp.dot(factor_wide, shrink[:, None] * projected, precision=lax.Precision.HIGHEST)
    solution = jnp.zeros_like(right_side)
    residual = right_side
    direction = precondition(residual)
    for iteration in range(ITERS):
        applied = apply_operator(design, direction)
        gram_block = inner_prod(direction, applied)
        gram_block = 0.5 * (gram_block + gram_block.T)
        chol_lower = jnp.linalg.cholesky(gram_block)
        unit_dir = jax.scipy.linalg.solve_triangular(chol_lower, direction.T, lower=True).T
        unit_img = jax.scipy.linalg.solve_triangular(chol_lower, applied.T, lower=True).T
        step_coef = jax.scipy.linalg.solve_triangular(chol_lower, inner_prod(direction, residual), lower=True)
        solution = solution + jnp.dot(unit_dir, step_coef, precision=lax.Precision.HIGHEST)
        residual = residual - jnp.dot(unit_img, step_coef, precision=lax.Precision.HIGHEST)
        if iteration + 1 < ITERS:
            scaled = precondition(residual)
            next_coef = -inner_prod(unit_img, scaled)
            direction = scaled + jnp.dot(unit_dir, next_coef, precision=lax.Precision.HIGHEST)
    return (solution, residual)
```

```python
import functools

import jax
import jax.numpy as jnp
from jax import lax
from jax.experimental import pallas as pl
from jax.experimental.pallas import tpu as pltpu
from jax.sharding import PartitionSpec as P

ITERS = 3

ridge_weight = 1.0

bf16 = jnp.bfloat16
f32 = jnp.float32
NT = (((1,), (1,)), ((), ()))
VMEM = pl.BlockSpec(memory_space=pltpu.VMEM)
HBM = pl.BlockSpec(memory_space=pl.ANY)
SMEM = pl.BlockSpec(memory_space=pltpu.SMEM)


def exact(left, right, dims=(((1,), (0,)), ((), ()))):
    return lax.dot_general(left, right, dims, precision=lax.Precision.HIGHEST, preferred_element_type=f32)


def with_narrow(values, narrow, dims):
    upper = values.astype(bf16)
    lower = (values - upper.astype(f32)).astype(bf16)
    first = lax.dot_general(upper, narrow, dims, preferred_element_type=f32)
    return first + lax.dot_general(lower, narrow, dims, preferred_element_type=f32)


def call(body, outs, args, specs, name, scratch=(), flops=0, bytes_accessed=0, limit=None):
    params = pltpu.CompilerParams(vmem_limit_bytes=limit) if limit else pltpu.CompilerParams()
    return pl.pallas_call(
        body,
        name=name,
        out_shape=[jax.ShapeDtypeStruct(shape, dtype) for shape, dtype in outs],
        in_specs=specs,
        out_specs=[VMEM] * len(outs),
        scratch_shapes=list(scratch),
        compiler_params=params,
        cost_estimate=pl.CostEstimate(flops=flops, bytes_accessed=bytes_accessed, transcendentals=0),
    )(*args)


def exchange(values, axis, size, mask):
    return lax.ppermute(values, axis, [(at, at ^ mask) for at in range(size)])


def stream_rows(design_ref, buffers, sems, first_sem, row_of, groups, per, tile, use):
    depth = buffers.shape[0]
    steps = groups * per
    half = tile // 2

    def copy(step):
        slot = lax.rem(step, depth)
        return pltpu.make_async_copy(
            design_ref.at[pl.ds(pl.multiple_of(row_of(step), tile), tile), :], buffers.at[slot], sems.at[slot]
        )

    def copy_half(side):
        return pltpu.make_async_copy(
            design_ref.at[pl.ds(pl.multiple_of(row_of(0) + side * half, half), half), :],
            buffers.at[0, pl.ds(side * half, half), :],
            first_sem.at[side],
        )

    def begin():
        copy_half(0).start()
        copy_half(1).start()
        for step in range(1, min(depth, steps)):
            copy(step).start()

    def run():
        for group in range(groups):
            if group == 0:
                for side in range(2):
                    copy_half(side).wait()
                    use(0, side * half, buffers[0, side * half : (side + 1) * half, :])
                if steps > depth:
                    copy(depth).start()

            def one(j, carry):
                step = group * per + j
                copy(step).wait()
                use(group, pl.multiple_of(j * tile, tile), buffers[lax.rem(step, depth)])

                @pl.when(step + depth < steps)
                def _():
                    copy(step + depth).start()

                return carry

            lax.fori_loop(1 if group == 0 else 0, per, one, 0)

    return begin, run


def place_shares(where, stacks, target, samples, rhs, width, turn):
    for across in range(rhs):
        for mask in range(samples):
            share = (where[2] ^ across) * samples + (where[1] ^ mask)
            start = pl.multiple_of(share * width, width)
            piece = stacks[across][mask]
            if turn:
                target[pl.ds(start, width), :] = jnp.swapaxes(piece.astype(f32), 0, 1).astype(target.dtype)
            else:
                target[:, pl.ds(start, width)] = piece


def forward_pass(where, stacks, design, masks, sizes):
    samples, feats, rhs = sizes
    rows, depth = design.shape
    cols = stacks[0].shape[1]
    chunk = rows // feats
    tile = min(256, chunk)
    per = chunk // tile
    width = depth // (samples * rhs)

    def body(where_ref, design_ref, *refs):
        stack_refs = refs[:rhs]
        outs = refs[rhs : rhs + len(masks)]
        buffers, turned, sems, first_sem = refs[rhs + len(masks) :]
        at = [where_ref[i] for i in range(3)]

        def row_of(step):
            return (at[0] ^ (masks[0] - step // per)) * chunk + lax.rem(step, per) * tile

        def use(group, start, block):
            out = jnp.dot(block, turned[...], preferred_element_type=f32)
            outs[group][:, pl.ds(start, block.shape[0])] = jnp.swapaxes(out, 0, 1).astype(bf16)

        begin, run = stream_rows(design_ref, buffers, sems, first_sem, row_of, len(masks), per, tile, use)
        begin()
        place_shares(at, stack_refs, turned, samples, rhs, width, True)
        run()

    work = len(masks) * chunk * depth
    return call(
        body,
        [((cols, chunk), bf16)] * len(masks),
        (where, design, *stacks),
        [SMEM, HBM] + [VMEM] * rhs,
        "forward",
        scratch=(
            pltpu.VMEM((4, tile, depth), bf16),
            pltpu.VMEM((depth, cols), bf16),
            pltpu.SemaphoreType.DMA((4,)),
            pltpu.SemaphoreType.DMA((2,)),
        ),
        flops=2 * work * cols,
        bytes_accessed=2 * work,
        limit=40 << 20,
    )


def backward_pass(where, pieces, design, masks, sizes, carried=None):
    samples, feats, rhs = sizes
    rows, depth = design.shape
    cols = pieces[0].shape[0]
    chunk = rows // feats
    tile = min(256, chunk)
    per = chunk // tile
    width = depth // (samples * rhs)
    n = len(masks)

    def body(where_ref, design_ref, *refs):
        piece_refs = refs[:n]
        last = carried is not None
        if last:
            start_ref, mine_ref, theirs_ref, buffers, total, sems, first_sem = refs[n:]
        else:
            total, buffers, sems, first_sem = refs[n:]
        at = [where_ref[i] for i in range(3)]

        def row_of(step):
            return (at[0] ^ (masks[0] + step // per)) * chunk + lax.rem(step, per) * tile

        def use(group, start, block):
            left = piece_refs[group][:, pl.ds(start, block.shape[0])]
            out = jnp.dot(left, block, preferred_element_type=f32)
            if group == 0 and isinstance(start, int) and start == 0:
                total[...] = start_ref[...] + out if last else out
            else:
                total[...] += out

        begin, run = stream_rows(design_ref, buffers, sems, first_sem, row_of, n, per, tile, use)
        begin()
        run()
        if last:
            for side, out in ((0, mine_ref), (1, theirs_ref)):
                for mask in range(samples):
                    share = (at[2] ^ side) * samples + (at[1] ^ mask)
                    out[mask] = total[:, pl.ds(pl.multiple_of(share * width, width), width)].astype(bf16)

    work = n * chunk * depth
    buffers = pltpu.VMEM((4, tile, depth), bf16)
    sems = (pltpu.SemaphoreType.DMA((4,)), pltpu.SemaphoreType.DMA((2,)))
    args = (where, design, *pieces)
    specs = [SMEM, HBM] + [VMEM] * n
    if carried is None:
        outs = [((cols, depth), f32)]
        scratch = (buffers, *sems)
    else:
        outs = [((samples, cols, width), bf16)] * 2
        args += (carried,)
        specs += [VMEM]
        scratch = (buffers, pltpu.VMEM((cols, depth), f32), *sems)
    return call(
        body, outs, args, specs, "backward", scratch=scratch, flops=2 * work * cols, bytes_accessed=2 * work, limit=40 << 20
    )


def merge(mine, theirs, samples, rhs, sent_dtype):
    came = exchange(theirs, "rhs", rhs, 1)
    sums = [mine[mask].astype(f32) + came[mask].astype(f32) for mask in range(samples)]
    return [sums[0]] + [one.astype(sent_dtype) for one in sums[1:]]


def sum_small(values, sizes):
    for axis, size in zip(("rhs", "samples", "features"), (sizes[2], sizes[0], sizes[1])):
        mask = 1
        while mask < size:
            values = values + exchange(values, axis, size, mask)
            mask *= 2
    return values


def share_all(values, samples, rhs):
    stack = jnp.stack([values] + [exchange(values, "samples", samples, mask) for mask in range(1, samples)])
    return [stack] + [exchange(stack, "rhs", rhs, mask) for mask in range(1, rhs)]


def sum_all(where, mine, theirs, sizes):
    samples, feats, rhs = sizes
    pieces = merge(mine, theirs, samples, rhs, f32)
    total = pieces[0]
    for mask in range(1, samples):
        total = total + exchange(pieces[mask], "samples", samples, mask)
    whole = total
    for mask in range(1, feats):
        whole = whole + exchange(total, "features", feats, mask)
    return share_all(whole, samples, rhs)


def write_halves(where_ref, packed, mine_ref, theirs_ref):
    samples, cols, width = mine_ref.shape
    for side, out in ((0, mine_ref), (1, theirs_ref)):
        for mask in range(samples):
            share = (where_ref[2] ^ side) * samples + (where_ref[1] ^ mask)
            out[mask] = packed[:, pl.ds(pl.multiple_of(share * width, width), width)]


def first_products(where, res, basis, wide, sizes):
    cols, rank = res.shape[0], basis.shape[1]

    def body(where_ref, res_ref, basis_ref, mine_ref, theirs_ref, packed):
        packed[...] = jnp.zeros_like(packed)
        packed[:, :rank] = with_narrow(res_ref[...], basis_ref[...], (((1,), (0,)), ((), ())))
        write_halves(where_ref, packed, mine_ref, theirs_ref)

    return call(
        body,
        [((sizes[0], cols, wide // (sizes[0] * sizes[2])), f32)] * 2,
        (where, res, basis),
        [SMEM, VMEM, VMEM],
        "first_products",
        scratch=(pltpu.VMEM((cols, wide), f32),),
    )


def first_update(where, stacks, res, basis, shrink, sizes):
    samples, feats, rhs = sizes
    cols, own = res.shape
    rank = basis.shape[1]
    width = stacks[0].shape[2]
    wide = width * samples * rhs

    def body(where_ref, *refs):
        stack_refs = refs[:rhs]
        res_ref, basis_ref, shrink_ref, proj_ref, dir_ref, narrow_ref, packed = refs[rhs:]
        at = [where_ref[i] for i in range(3)]
        place_shares(at, stack_refs, packed, samples, rhs, width, False)
        proj = packed[:, :rank]
        proj_ref[...] = proj
        direction = res_ref[...] + with_narrow(proj * shrink_ref[...], basis_ref[...], NT)
        dir_ref[...] = direction
        narrow_ref[...] = direction.astype(bf16)

    return call(
        body,
        [((cols, rank), f32), ((cols, own), f32), ((cols, own), bf16)],
        (where, *stacks, res, basis, shrink),
        [SMEM] + [VMEM] * (rhs + 3),
        "first_update",
        scratch=(pltpu.VMEM((cols, wide), f32),),
    )


def products(where, kept, arrived, direction, res, basis, wide, sizes):
    cols, own = res.shape
    rank = basis.shape[1]
    n = len(arrived)

    def body(where_ref, kept_ref, *refs):
        arrived_refs = refs[:n]
        dir_ref, res_ref, basis_ref, applied_ref, mine_ref, theirs_ref, packed = refs[n:]
        applied = kept_ref[...]
        for ref in arrived_refs:
            applied = applied + ref[...].astype(f32)
        direction_now, residual = dir_ref[...], res_ref[...]
        applied = applied + ridge_weight * direction_now
        applied_ref[...] = applied
        packed[...] = jnp.zeros_like(packed)
        packed[:, rank : rank + cols] = exact(direction_now, applied, NT)
        packed[:, rank + cols : rank + 2 * cols] = exact(residual, direction_now, NT)
        packed[:, :rank] = with_narrow(applied, basis_ref[...], (((1,), (0,)), ((), ())))
        packed[:, rank + 2 * cols : rank + 3 * cols] = exact(applied, applied, NT)
        packed[:, rank + 3 * cols : rank + 4 * cols] = exact(residual, applied, NT)
        write_halves(where_ref, packed, mine_ref, theirs_ref)

    return call(
        body,
        [((cols, own), f32)] + [((sizes[0], cols, wide // (sizes[0] * sizes[2])), f32)] * 2,
        (where, kept, *arrived, direction, res, basis),
        [SMEM] + [VMEM] * (n + 4),
        "products",
        scratch=(pltpu.VMEM((cols, wide), f32),),
    )


def inverse(matrix):
    size = matrix.shape[0]
    row_at = lax.broadcasted_iota(jnp.int32, (size, 1), 0)
    unit = lax.broadcasted_iota(jnp.int32, (size, size), 0) == lax.broadcasted_iota(jnp.int32, (size, size), 1)
    work = jnp.concatenate([matrix, unit.astype(f32)], axis=1)
    for k in range(size):
        row = work[k : k + 1, :]
        recip = 1.0 / row[:, k : k + 1]
        column = work[:, k : k + 1]
        scale = jnp.where(row_at == k, 1.0 - recip, column * recip)
        work = work - scale * row
    return work[:, size:]


def update(where, stacks, proj, direction, applied, res, basis, shrink, sizes):
    samples, feats, rhs = sizes
    cols, own = res.shape
    rank = basis.shape[1]
    width = stacks[0].shape[2]
    wide = width * samples * rhs

    def body(where_ref, *refs):
        stack_refs = refs[:rhs]
        proj_ref, dir_ref, applied_ref, res_ref, basis_ref, shrink_ref, step_ref, new_res_ref = refs[rhs : rhs + 8]
        packed = refs[-1]
        at = [where_ref[i] for i in range(3)]
        place_shares(at, stack_refs, packed, samples, rhs, width, False)
        gram = packed[:, rank : rank + cols]
        gram = 0.5 * (gram + jnp.swapaxes(gram, 0, 1))
        inv = inverse(gram)
        inv = 0.5 * (inv + jnp.swapaxes(inv, 0, 1))
        step = exact(packed[:, rank + cols : rank + 2 * cols], inv)
        step_ref[...] = step
        residual = res_ref[...] - exact(step, applied_ref[...])
        new_res_ref[...] = residual
        new_proj_ref, new_dir_ref, narrow_ref = refs[rhs + 8 : -1]
        image = packed[:, :rank]
        new_proj = proj_ref[...] - exact(step, image)
        new_proj_ref[...] = new_proj
        scaled = new_proj * shrink_ref[...]
        cross = packed[:, rank + 3 * cols : rank + 4 * cols] - exact(step, packed[:, rank + 2 * cols : rank + 3 * cols])
        cross = cross + exact(scaled, image, NT)
        next_coef = -exact(cross, inv)
        new_dir = residual + with_narrow(scaled, basis_ref[...], NT) + exact(next_coef, dir_ref[...])
        new_dir_ref[...] = new_dir
        narrow_ref[...] = new_dir.astype(bf16)

    outs = [((cols, cols), f32), ((cols, own), f32)]
    outs += [((cols, rank), f32), ((cols, own), f32), ((cols, own), bf16)]
    return call(
        body,
        outs,
        (where, *stacks, proj, direction, applied, res, basis, shrink),
        [SMEM] + [VMEM] * (rhs + 6),
        "update",
        scratch=(pltpu.VMEM((cols, wide), f32),),
    )


def gram_part(kept, came, direction, res):
    cols, chunk = kept.shape
    n = len(came)

    def body(kept_ref, *refs):
        dir_ref, res_ref, image_ref, gram_ref = refs[n:]
        total = kept_ref[...].astype(f32)
        for ref in refs[:n]:
            total = total + ref[...].astype(f32)
        image = total.astype(bf16)
        image_ref[...] = image
        direction_now = dir_ref[...]
        gram = exact(total, image.astype(f32), NT) + ridge_weight * exact(direction_now, direction_now, NT)
        gram_ref[:, :cols] = gram
        gram_ref[:, cols:] = exact(res_ref[...], direction_now, NT)

    return call(
        body, [((cols, chunk), bf16), ((cols, 2 * cols), f32)], (kept, *came, direction, res), [VMEM] * (n + 3), "gram_part"
    )


def last_step(grams):
    cols = grams.shape[0]

    def body(gram_ref, step_ref):
        gram = gram_ref[:, :cols]
        inv = inverse(0.5 * (gram + jnp.swapaxes(gram, 0, 1)))
        step_ref[...] = exact(gram_ref[:, cols:], 0.5 * (inv + jnp.swapaxes(inv, 0, 1)))

    return call(body, [((cols, cols), f32)], (grams,), [VMEM], "last_step")[0]


def last_residual(where, kept, arrived, direction, res, step, part):
    cols, own = res.shape
    n = len(arrived)

    def body(where_ref, kept_ref, *refs):
        dir_ref, res_ref, step_ref, same_ref, other_ref, whole = refs[n:]
        applied = kept_ref[...]
        for ref in refs[:n]:
            applied = applied + ref[...].astype(f32)
        applied = applied + ridge_weight * dir_ref[...]
        whole[...] = res_ref[...] - exact(step_ref[...], applied)
        same_ref[...] = whole[pl.ds(pl.multiple_of(where_ref[2] * part, part), part), :].astype(bf16)
        other_ref[...] = whole[pl.ds(pl.multiple_of((where_ref[2] ^ 1) * part, part), part), :].astype(bf16)

    return call(
        body,
        [((part, own), bf16)] * 2,
        (where, kept, *arrived, direction, res, step),
        [SMEM] + [VMEM] * (n + 4),
        "last_residual",
        scratch=(pltpu.VMEM((cols, own), f32),),
    )


def collect(where, all_stacks, steps, sizes):
    samples, feats, rhs = sizes
    cols, width = all_stacks[0][0].shape[1:]
    part = cols // rhs
    count = len(all_stacks)
    depth = width * samples * rhs

    def body(where_ref, *refs):
        stack_refs, step_refs, out_ref = refs[: count * rhs], refs[count * rhs : -1], refs[-1]
        at = [where_ref[i] for i in range(3)]
        rows = pl.ds(pl.multiple_of(at[2] * part, part), part)
        coefs = [ref[rows, :] for ref in step_refs]
        for across in range(rhs):
            for mask in range(samples):
                share = (at[2] ^ across) * samples + (at[1] ^ mask)
                total = jnp.zeros((part, width), f32)
                for k in range(count):
                    upper = coefs[k].astype(bf16)
                    lower = (coefs[k] - upper.astype(f32)).astype(bf16)
                    block = stack_refs[k * rhs + across][mask]
                    total += jnp.dot(upper, block, preferred_element_type=f32)
                    total += jnp.dot(lower, block, preferred_element_type=f32)
                out_ref[:, pl.ds(pl.multiple_of(share * width, width), width)] = total

    return call(
        body,
        [((part, depth), f32)],
        (where, *[one for stacks in all_stacks for one in stacks], *steps),
        [SMEM] + [VMEM] * (count * rhs + count),
        "collect",
    )[0]


def shards(sizes, design, right_side, factor, nystrom_values):
    samples, feats, rhs = sizes
    depth, col_share = right_side.shape
    own = depth // (samples * rhs)
    at_sample, at_feat, at_rhs = lax.axis_index("samples"), lax.axis_index("features"), lax.axis_index("rhs")
    where = jnp.stack([at_feat, at_sample, at_rhs]).astype(jnp.int32)
    shrink = ((1.0 + jnp.min(nystrom_values)) / (1.0 + nystrom_values) - 1.0)[None, :]
    rank = shrink.shape[1]
    cols = col_share * rhs
    unit = 128 * samples * rhs
    wide = -(-(rank + 4 * cols) // unit) * unit

    def own_rows(block):
        mine = lax.dynamic_slice_in_dim(block, (at_rhs * samples + at_sample) * own, own, 0)
        theirs = lax.dynamic_slice_in_dim(block, ((1 - at_rhs) * samples + at_sample) * own, own, 0)
        came = exchange(theirs, "rhs", rhs, 1)
        return jnp.where(at_rhs == 0, jnp.concatenate([mine, came], 1), jnp.concatenate([came, mine], 1))

    res = own_rows(right_side).T
    basis = own_rows(factor)
    proj_stacks = sum_all(where, *first_products(where, res, basis, wide, sizes), sizes)
    proj, direction, narrow = first_update(where, proj_stacks, res, basis, shrink, sizes)
    all_stacks, steps = [], []
    for iteration in range(ITERS):
        last = iteration + 1 == ITERS
        stacks = share_all(narrow, samples, rhs)
        all_stacks.append(stacks)
        away = list(range(feats - 1, 0, -1))
        sent = forward_pass(where, stacks, design, away, sizes)
        came = [exchange(value, "features", feats, mask) for value, mask in zip(sent, away)]
        (kept,) = forward_pass(where, stacks, design, [0], sizes)
        if last:
            image, grams = gram_part(kept, came, direction, res)
            grams = sum_small(grams, sizes)
        else:
            total = kept.astype(f32)
            for value in came:
                total = total + value.astype(f32)
            image = total.astype(bf16)
        others = [exchange(image, "features", feats, mask) for mask in range(1, feats)]
        (carried,) = backward_pass(where, [image], design, [0], sizes)
        mine, theirs = backward_pass(where, others, design, list(range(1, feats)), sizes, carried)
        pieces = merge(mine, theirs, samples, rhs, bf16)
        arrived = [exchange(pieces[mask], "samples", samples, mask) for mask in range(1, samples)]
        if last:
            step = last_step(grams)
            same, other = last_residual(where, pieces[0], arrived, direction, res, step, col_share)
        else:
            applied, *halves = products(where, pieces[0], arrived, direction, res, basis, wide, sizes)
            sums = sum_all(where, *halves, sizes)
            step, res, proj, direction, narrow = update(
                where, sums, proj, direction, applied, res, basis, shrink, sizes
            )
        steps.append(step)
    pair = jnp.stack([same, exchange(other, "rhs", rhs, 1)])
    parts = jnp.stack([pair] + [exchange(pair, "samples", samples, mask) for mask in range(1, samples)])
    out_sol = collect(where, all_stacks, steps, sizes).T
    order = jnp.arange(samples) ^ at_sample
    sides = jnp.arange(rhs) ^ at_rhs
    parts = parts[order][:, sides]
    out_res = parts.transpose(1, 0, 3, 2).reshape(depth, col_share).astype(f32)
    return (out_sol, out_res)


def solution(mesh):
    sizes = (mesh.shape["samples"], mesh.shape["features"], mesh.shape["rhs"])
    placed = (P(("samples", "rhs"), "features"), P("features", "rhs"), P("features", "rhs"), P())
    return jax.shard_map(
        functools.partial(shards, sizes),
        mesh=mesh,
        in_specs=placed,
        out_specs=(P("features", "rhs"), P("features", "rhs")),
        check_vma=False,
    )
```

```python
import functools

import jax
import jax.numpy as jnp
from jax import lax
from jax.experimental import pallas as pl
from jax.experimental.pallas import tpu as pltpu
from jax.sharding import PartitionSpec as P


ITERS = 3

ridge_weight = 1.0

bf16 = jnp.bfloat16
f32 = jnp.float32
NT = (((1,), (1,)), ((), ()))
VMEM = pl.BlockSpec(memory_space=pltpu.VMEM)
HBM = pl.BlockSpec(memory_space=pl.ANY)
SMEM = pl.BlockSpec(memory_space=pltpu.SMEM)


def exact(left, right, dims=(((1,), (0,)), ((), ()))):
    return lax.dot_general(left, right, dims, precision=lax.Precision.HIGHEST, preferred_element_type=f32)


def with_narrow(values, narrow, dims):
    upper = values.astype(bf16)
    lower = (values - upper.astype(f32)).astype(bf16)
    first = lax.dot_general(upper, narrow, dims, preferred_element_type=f32)
    return first + lax.dot_general(lower, narrow, dims, preferred_element_type=f32)


def call(body, outs, args, specs, scratch=(), flops=0, bytes_accessed=0, limit=None):
    params = pltpu.CompilerParams(vmem_limit_bytes=limit) if limit else pltpu.CompilerParams()
    return pl.pallas_call(
        body,
        out_shape=[jax.ShapeDtypeStruct(shape, dtype) for shape, dtype in outs],
        in_specs=specs,
        out_specs=[VMEM] * len(outs),
        scratch_shapes=list(scratch),
        compiler_params=params,
        cost_estimate=pl.CostEstimate(flops=flops, bytes_accessed=bytes_accessed, transcendentals=0),
    )(*args)


def exchange(values, axis, size, mask):
    return lax.ppermute(values, axis, [(at, at ^ mask) for at in range(size)])


def stream_rows(design_ref, buffers, sems, row_of, steps, tile, use):
    depth = buffers.shape[0]

    def copy(step):
        slot = lax.rem(step, depth)
        return pltpu.make_async_copy(
            design_ref.at[pl.ds(pl.multiple_of(row_of(step), tile), tile), :], buffers.at[slot], sems.at[slot]
        )

    def begin():
        for step in range(min(depth, steps)):
            copy(step).start()

    def run():
        def one(step, carry):
            copy(step).wait()
            use(step, buffers[lax.rem(step, depth)])

            @pl.when(step + depth < steps)
            def _():
                copy(step + depth).start()

            return carry

        lax.fori_loop(0, steps, one, 0)

    return begin, run


def place_shares(where, stacks, target, samples, rhs, width):
    for across in range(rhs):
        for mask in range(samples):
            share = (where[2] ^ across) * samples + (where[1] ^ mask)
            target[:, pl.ds(pl.multiple_of(share * width, width), width)] = stacks[across][mask]


def times_columns(block, left):
    pieces = 4
    width = left.shape[1] // pieces
    cut = width * 3 // 4 if width * 3 % 1024 == 0 else width // 2
    streamed, held = None, None
    for start in range(0, pieces * width, width):
        one = lax.dot_general(block[:, start : start + cut], left[:, start : start + cut], NT, preferred_element_type=f32)
        span = slice(start + cut, start + width)
        two = lax.dot_general(left[:, span], block[:, span], NT, preferred_element_type=f32)
        streamed = one if streamed is None else streamed + one
        held = two if held is None else held + two
    return jnp.swapaxes(streamed, 0, 1) + held


def forward_pass(where, stacks, design, masks, sizes):
    samples, feats, rhs = sizes
    rows, depth = design.shape
    cols = stacks[0].shape[1]
    chunk = rows // feats
    tile = min(256, chunk)
    per = chunk // tile
    width = depth // (samples * rhs)

    def body(where_ref, design_ref, *refs):
        stack_refs = refs[:rhs]
        outs = refs[rhs : rhs + len(masks)]
        buffers, joined, sems = refs[rhs + len(masks) :]
        at = [where_ref[i] for i in range(3)]

        def row_of(step):
            return (at[0] ^ (masks[0] - step // per)) * chunk + lax.rem(step, per) * tile

        def use(step, block):
            out = times_columns(block, joined[...]).astype(bf16)
            start = pl.multiple_of(lax.rem(step, per) * tile, tile)
            for group in range(len(masks)):

                @pl.when(step // per == group)
                def _(group=group):
                    outs[group][:, pl.ds(start, tile)] = out

        begin, run = stream_rows(design_ref, buffers, sems, row_of, len(masks) * per, tile, use)
        begin()
        place_shares(at, stack_refs, joined, samples, rhs, width)
        run()

    work = len(masks) * chunk * depth
    return call(
        body,
        [((cols, chunk), bf16)] * len(masks),
        (where, design, *stacks),
        [SMEM, HBM] + [VMEM] * rhs,
        scratch=(
            pltpu.VMEM((4, tile, depth), bf16),
            pltpu.VMEM((cols, depth), bf16),
            pltpu.SemaphoreType.DMA((4,)),
        ),
        flops=2 * work * cols,
        bytes_accessed=2 * work,
        limit=40 << 20,
    )


def backward_pass(where, pieces, design, masks, sizes, carried=None):
    samples, feats, rhs = sizes
    rows, depth = design.shape
    cols = pieces[0].shape[0]
    chunk = rows // feats
    tile = min(256, chunk)
    per = chunk // tile
    width = depth // (samples * rhs)
    n = len(masks)

    def body(where_ref, design_ref, *refs):
        piece_refs = refs[:n]
        last = carried is not None
        if last:
            start_ref, mine_ref, theirs_ref, buffers, joined, sems, total = refs[n:]
        else:
            total, buffers, joined, sems = refs[n:]
        at = [where_ref[i] for i in range(3)]

        def row_of(step):
            return (at[0] ^ (masks[0] + step // per)) * chunk + lax.rem(step, per) * tile

        def use(step, block):
            left = joined[:, pl.ds(pl.multiple_of(step * tile, tile), tile)]
            total[...] += jnp.dot(left, block, preferred_element_type=f32)

        begin, run = stream_rows(design_ref, buffers, sems, row_of, n * per, tile, use)
        begin()
        for group in range(n):
            joined[:, group * chunk : (group + 1) * chunk] = piece_refs[group][...]
        total[...] = start_ref[...] if last else jnp.zeros_like(total)
        run()
        if last:
            for side, out in ((0, mine_ref), (1, theirs_ref)):
                for mask in range(samples):
                    share = (at[2] ^ side) * samples + (at[1] ^ mask)
                    out[mask] = total[:, pl.ds(pl.multiple_of(share * width, width), width)].astype(bf16)

    work = n * chunk * depth
    buffers = pltpu.VMEM((4, tile, depth), bf16)
    sems = (pltpu.VMEM((cols, n * chunk), bf16), pltpu.SemaphoreType.DMA((4,)))
    args = (where, design, *pieces)
    specs = [SMEM, HBM] + [VMEM] * n
    if carried is None:
        outs = [((cols, depth), f32)]
        scratch = (buffers, *sems)
    else:
        outs = [((samples, cols, width), bf16)] * 2
        args += (carried,)
        specs += [VMEM]
        scratch = (buffers, *sems, pltpu.VMEM((cols, depth), f32))
    return call(
        body, outs, args, specs, scratch=scratch, flops=2 * work * cols, bytes_accessed=2 * work, limit=40 << 20
    )


def merge(mine, theirs, samples, rhs, sent_dtype):
    came = exchange(theirs, "rhs", rhs, 1)
    sums = [mine[mask].astype(f32) + came[mask].astype(f32) for mask in range(samples)]
    return [sums[0]] + [one.astype(sent_dtype) for one in sums[1:]]


def sum_small(values, sizes):
    for axis, size in zip(("samples", "features", "rhs"), sizes):
        came = [exchange(values, axis, size, mask) for mask in range(1, size)]
        for one in came:
            values = values + one
    return values


def sum_features(total, size):
    whole = total
    for mask in range(1, size):
        whole = whole + exchange(total, "features", size, mask)
    return whole


def share_all(values, samples, rhs):
    stack = jnp.stack([values] + [exchange(values, "samples", samples, mask) for mask in range(1, samples)])
    return [stack] + [exchange(stack, "rhs", rhs, mask) for mask in range(1, rhs)]


def sum_all(mine, theirs, sizes):
    samples, feats, rhs = sizes
    pieces = merge(mine, theirs, samples, rhs, f32)
    total = pieces[0]
    for mask in range(1, samples):
        total = total + exchange(pieces[mask], "samples", samples, mask)
    return share_all(sum_features(total, feats), samples, rhs)


def write_halves(where_ref, packed, mine_ref, theirs_ref):
    samples, _, width = mine_ref.shape
    for side, out in ((0, mine_ref), (1, theirs_ref)):
        for mask in range(samples):
            share = (where_ref[2] ^ side) * samples + (where_ref[1] ^ mask)
            out[mask] = packed[:, pl.ds(pl.multiple_of(share * width, width), width)]


def first_products(where, near, far, factor, width):
    part, depth = near.shape
    last_start = factor.shape[1] - width

    def body(where_ref, near_ref, far_ref, factor_ref, out_ref, share_ref, sem):
        start = pl.multiple_of(jnp.minimum(where_ref[1] * width, last_start), width)
        copy = pltpu.make_async_copy(factor_ref.at[:, pl.ds(start, width)], share_ref, sem)
        copy.start()
        copy.wait()
        for side, ref in ((0, near_ref), (1, far_ref)):
            found = with_narrow(ref[...], share_ref[...], (((1,), (0,)), ((), ())))
            out_ref[pl.ds(pl.multiple_of((where_ref[2] ^ side) * part, part), part), :] = found

    return call(
        body,
        [((2 * part, width), f32)],
        (where, near, far, factor),
        [SMEM, VMEM, VMEM, HBM],
        scratch=(pltpu.VMEM((depth, width), bf16), pltpu.SemaphoreType.DMA),
    )[0]


def first_update(where, stacks, res, basis, shrink, sizes):
    samples, _, rhs = sizes
    cols, own = res.shape
    rank = basis.shape[1]
    width = stacks[0].shape[2]
    wide = width * samples * rhs

    def body(where_ref, *refs):
        stack_refs = refs[:rhs]
        res_ref, basis_ref, shrink_ref, proj_ref, dir_ref, narrow_ref, packed = refs[rhs:]
        at = [where_ref[i] for i in range(3)]
        place_shares(at, stack_refs, packed, samples, rhs, width)
        side = wide // rhs
        for across in range(rhs):
            proj_ref[:, across * (rank // rhs) : (across + 1) * (rank // rhs)] = packed[:, across * side : across * side + rank // rhs]
        proj = proj_ref[...]
        direction = res_ref[...] + with_narrow(proj * shrink_ref[...], basis_ref[...], NT)
        dir_ref[...] = direction
        narrow_ref[...] = direction.astype(bf16)

    return call(
        body,
        [((cols, rank), f32), ((cols, own), f32), ((cols, own), bf16)],
        (where, *stacks, res, basis, shrink),
        [SMEM] + [VMEM] * (rhs + 3),
        scratch=(pltpu.VMEM((cols, wide), f32),),
    )


def products(where, kept, arrived, direction, res, basis, wide, sizes):
    cols, own = res.shape
    rank = basis.shape[1]
    n = len(arrived)

    def body(where_ref, kept_ref, *refs):
        arrived_refs = refs[:n]
        dir_ref, res_ref, basis_ref, applied_ref, mine_ref, theirs_ref, packed = refs[n:]
        applied = kept_ref[...]
        for ref in arrived_refs:
            applied = applied + ref[...].astype(f32)
        direction_now, residual = dir_ref[...], res_ref[...]
        applied = applied + ridge_weight * direction_now
        applied_ref[...] = applied
        packed[...] = jnp.zeros_like(packed)
        packed[:, rank : rank + cols] = exact(direction_now, applied, NT)
        packed[:, rank + cols : rank + 2 * cols] = exact(residual, direction_now, NT)
        packed[:, :rank] = with_narrow(applied, basis_ref[...], (((1,), (0,)), ((), ())))
        packed[:, rank + 2 * cols : rank + 3 * cols] = exact(applied, applied, NT)
        packed[:, rank + 3 * cols : rank + 4 * cols] = exact(residual, applied, NT)
        write_halves(where_ref, packed, mine_ref, theirs_ref)

    return call(
        body,
        [((cols, own), f32)] + [((sizes[0], cols, wide // (sizes[0] * sizes[2])), f32)] * 2,
        (where, kept, *arrived, direction, res, basis),
        [SMEM] + [VMEM] * (n + 4),
        scratch=(pltpu.VMEM((cols, wide), f32),),
    )


def inverse(matrix):
    size = matrix.shape[0]
    row_at = lax.broadcasted_iota(jnp.int32, (size, 1), 0)
    unit = lax.broadcasted_iota(jnp.int32, (size, size), 0) == lax.broadcasted_iota(jnp.int32, (size, size), 1)
    work = jnp.concatenate([matrix, unit.astype(f32)], axis=1)
    for k in range(size):
        recip = 1.0 / work[k : k + 1, k : k + 1]
        row = work[k : k + 1, :] * recip
        work = jnp.where(row_at == k, row, work - work[:, k : k + 1] * row)
    return work[:, size:]


def update(where, stacks, proj, direction, applied, res, basis, shrink, sizes):
    samples, _, rhs = sizes
    cols, own = res.shape
    rank = basis.shape[1]
    width = stacks[0].shape[2]
    wide = width * samples * rhs

    def body(where_ref, *refs):
        stack_refs = refs[:rhs]
        proj_ref, dir_ref, applied_ref, res_ref, basis_ref, shrink_ref, step_ref, new_res_ref = refs[rhs : rhs + 8]
        packed = refs[-1]
        at = [where_ref[i] for i in range(3)]
        place_shares(at, stack_refs, packed, samples, rhs, width)
        gram = packed[:, rank : rank + cols]
        gram = 0.5 * (gram + jnp.swapaxes(gram, 0, 1))
        inv = inverse(gram)
        inv = 0.5 * (inv + jnp.swapaxes(inv, 0, 1))
        step = exact(packed[:, rank + cols : rank + 2 * cols], inv)
        step_ref[...] = step
        residual = res_ref[...] - exact(step, applied_ref[...])
        new_res_ref[...] = residual
        new_proj_ref, new_dir_ref, narrow_ref = refs[rhs + 8 : -1]
        image = packed[:, :rank]
        new_proj = proj_ref[...] - exact(step, image)
        new_proj_ref[...] = new_proj
        scaled = new_proj * shrink_ref[...]
        cross = packed[:, rank + 3 * cols : rank + 4 * cols] - exact(step, packed[:, rank + 2 * cols : rank + 3 * cols])
        cross = cross + exact(scaled, image, NT)
        next_coef = -exact(cross, inv)
        new_dir = residual + with_narrow(scaled, basis_ref[...], NT) + exact(next_coef, dir_ref[...])
        new_dir_ref[...] = new_dir
        narrow_ref[...] = new_dir.astype(bf16)

    outs = [((cols, cols), f32), ((cols, own), f32)]
    outs += [((cols, rank), f32), ((cols, own), f32), ((cols, own), bf16)]
    return call(
        body,
        outs,
        (where, *stacks, proj, direction, applied, res, basis, shrink),
        [SMEM] + [VMEM] * (rhs + 6),
        scratch=(pltpu.VMEM((cols, wide), f32),),
    )


def gram_part(kept, came, direction, res):
    cols, chunk = kept.shape
    n = len(came)

    def body(kept_ref, *refs):
        dir_ref, res_ref, image_ref, gram_ref = refs[n:]
        total = kept_ref[...].astype(f32)
        for ref in refs[:n]:
            total = total + ref[...].astype(f32)
        image = total.astype(bf16)
        image_ref[...] = image
        direction_now = dir_ref[...]
        gram = exact(total, image.astype(f32), NT) + ridge_weight * exact(direction_now, direction_now, NT)
        gram_ref[:, :cols] = gram
        gram_ref[:, cols:] = exact(res_ref[...], direction_now, NT)

    return call(body, [((cols, chunk), bf16), ((cols, 2 * cols), f32)], (kept, *came, direction, res), [VMEM] * (n + 3))


def last_step(grams):
    cols = grams.shape[0]

    def body(gram_ref, step_ref):
        gram = gram_ref[:, :cols]
        inv = inverse(0.5 * (gram + jnp.swapaxes(gram, 0, 1)))
        step_ref[...] = exact(gram_ref[:, cols:], 0.5 * (inv + jnp.swapaxes(inv, 0, 1)))

    return call(body, [((cols, cols), f32)], (grams,), [VMEM], flops=10**9)[0]


def last_residual(where, kept, arrived, direction, res, step, part):
    cols, own = res.shape
    n = len(arrived)

    def body(where_ref, kept_ref, *refs):
        dir_ref, res_ref, step_ref, same_ref, other_ref, whole = refs[n:]
        applied = kept_ref[...]
        for ref in refs[:n]:
            applied = applied + ref[...].astype(f32)
        applied = applied + ridge_weight * dir_ref[...]
        whole[...] = res_ref[...] - exact(step_ref[...], applied)
        same_ref[...] = whole[pl.ds(pl.multiple_of(where_ref[2] * part, part), part), :].astype(bf16)
        other_ref[...] = whole[pl.ds(pl.multiple_of((where_ref[2] ^ 1) * part, part), part), :].astype(bf16)

    return call(
        body,
        [((part, own), bf16)] * 2,
        (where, kept, *arrived, direction, res, step),
        [SMEM] + [VMEM] * (n + 4),
        scratch=(pltpu.VMEM((cols, own), f32),),
    )


def collect(where, all_stacks, steps, sizes):
    samples, _, rhs = sizes
    cols, width = all_stacks[0][0].shape[1:]
    part = cols // rhs
    count = len(all_stacks)
    depth = width * samples * rhs

    def body(where_ref, *refs):
        stack_refs, step_refs, out_ref = refs[: count * rhs], refs[count * rhs : -1], refs[-1]
        at = [where_ref[i] for i in range(3)]
        rows = pl.ds(pl.multiple_of(at[2] * part, part), part)
        coefs = [ref[rows, :] for ref in step_refs]
        for across in range(rhs):
            for mask in range(samples):
                share = (at[2] ^ across) * samples + (at[1] ^ mask)
                total = jnp.zeros((part, width), f32)
                for k in range(count):
                    upper = coefs[k].astype(bf16)
                    lower = (coefs[k] - upper.astype(f32)).astype(bf16)
                    block = stack_refs[k * rhs + across][mask]
                    total += jnp.dot(upper, block, preferred_element_type=f32)
                    total += jnp.dot(lower, block, preferred_element_type=f32)
                out_ref[:, pl.ds(pl.multiple_of(share * width, width), width)] = total

    return call(
        body,
        [((part, depth), f32)],
        (where, *[one for stacks in all_stacks for one in stacks], *steps),
        [SMEM] + [VMEM] * (count * rhs + count),
    )[0]


def shards(sizes, design, right_side, factor, nystrom_values):
    samples, feats, rhs = sizes
    depth, col_share = right_side.shape
    own = depth // (samples * rhs)
    at_sample, at_feat, at_rhs = lax.axis_index("samples"), lax.axis_index("features"), lax.axis_index("rhs")
    where = jnp.stack([at_feat, at_sample, at_rhs]).astype(jnp.int32)
    shrink = ((1.0 + jnp.min(nystrom_values)) / (1.0 + nystrom_values) - 1.0)[None, :]
    rank = shrink.shape[1]
    cols = col_share * rhs
    unit = 128 * samples * rhs
    wide = -(-(rank + 4 * cols) // unit) * unit

    share = at_rhs * samples + at_sample
    other_share = (1 - at_rhs) * samples + at_sample
    near = right_side.T
    far = exchange(near, "rhs", rhs, 1)
    found = sum_features(first_products(where, near, far, factor, wide // (samples * rhs)), feats)
    proj_stacks = share_all(found, samples, rhs)
    own_near = lax.dynamic_slice_in_dim(near, share * own, own, 1)
    own_far = lax.dynamic_slice_in_dim(far, share * own, own, 1)
    res = jnp.where(at_rhs == 0, jnp.concatenate([own_near, own_far]), jnp.concatenate([own_far, own_near]))
    mine = lax.dynamic_slice_in_dim(factor, share * own, own, 0)
    came = exchange(lax.dynamic_slice_in_dim(factor, other_share * own, own, 0), "rhs", rhs, 1)
    basis = jnp.where(at_rhs == 0, jnp.concatenate([mine, came], 1), jnp.concatenate([came, mine], 1))
    proj, direction, narrow = first_update(where, proj_stacks, res, basis, shrink, sizes)
    all_stacks, steps = [], []
    for iteration in range(ITERS):
        last = iteration + 1 == ITERS
        stacks = share_all(narrow, samples, rhs)
        all_stacks.append(stacks)
        away = list(range(feats - 1, 0, -1))
        sent = forward_pass(where, stacks, design, away, sizes)
        came = [exchange(value, "features", feats, mask) for value, mask in zip(sent, away)]
        (kept,) = forward_pass(where, stacks, design, [0], sizes)
        if last:
            image, grams = gram_part(kept, came, direction, res)
            grams = sum_small(grams, sizes)
        else:
            total = kept.astype(f32)
            for value in came:
                total = total + value.astype(f32)
            image = total.astype(bf16)
        others = [exchange(image, "features", feats, mask) for mask in range(1, feats)]
        (carried,) = backward_pass(where, [image], design, [0], sizes)
        mine, theirs = backward_pass(where, others, design, list(range(1, feats)), sizes, carried)
        pieces = merge(mine, theirs, samples, rhs, bf16)
        arrived = [exchange(pieces[mask], "samples", samples, mask) for mask in range(1, samples)]
        if last:
            step = last_step(grams)
            same, other = last_residual(where, pieces[0], arrived, direction, res, step, col_share)
        else:
            applied, *halves = products(where, pieces[0], arrived, direction, res, basis, wide, sizes)
            sums = sum_all(*halves, sizes)
            step, res, proj, direction, narrow = update(
                where, sums, proj, direction, applied, res, basis, shrink, sizes
            )
        steps.append(step)
    pair = jnp.stack([same, exchange(other, "rhs", rhs, 1)])
    parts = jnp.stack([pair] + [exchange(pair, "samples", samples, mask) for mask in range(1, samples)])
    out_sol = collect(where, all_stacks, steps, sizes).T
    order = jnp.arange(samples) ^ at_sample
    sides = jnp.arange(rhs) ^ at_rhs
    parts = parts[order][:, sides]
    out_res = parts.transpose(1, 0, 3, 2).reshape(depth, col_share).astype(f32)
    return (out_sol, out_res)


def solution(mesh):
    sizes = (mesh.shape["samples"], mesh.shape["features"], mesh.shape["rhs"])
    placed = (P(("samples", "rhs"), "features"), P("features", "rhs"), P("features", "rhs"), P())
    return jax.shard_map(
        functools.partial(shards, sizes),
        mesh=mesh,
        in_specs=placed,
        out_specs=(P("features", "rhs"), P("features", "rhs")),
        check_vma=False,
    )
```

```python
import functools

import jax
import jax.numpy as jnp
from jax import lax
from jax.experimental import pallas as pl
from jax.experimental.pallas import tpu as pltpu
from jax.sharding import PartitionSpec as P


ITERS = 3

ridge_weight = 1.0

bf16 = jnp.bfloat16
f32 = jnp.float32
NT = (((1,), (1,)), ((), ()))
VMEM = pl.BlockSpec(memory_space=pltpu.VMEM)
HBM = pl.BlockSpec(memory_space=pl.ANY)
SMEM = pl.BlockSpec(memory_space=pltpu.SMEM)


def exact(left, right, dims=(((1,), (0,)), ((), ()))):
    return lax.dot_general(left, right, dims, precision=lax.Precision.HIGHEST, preferred_element_type=f32)


def with_narrow(values, narrow, dims):
    upper = values.astype(bf16)
    lower = (values - upper.astype(f32)).astype(bf16)
    both = lax.dot_general(jnp.concatenate([upper, lower]), narrow, dims, preferred_element_type=f32)
    return both[: values.shape[0]] + both[values.shape[0] :]


def call(body, outs, args, specs, scratch=(), flops=0, bytes_accessed=0, limit=None):
    params = pltpu.CompilerParams(vmem_limit_bytes=limit) if limit else pltpu.CompilerParams()
    return pl.pallas_call(
        body,
        out_shape=[jax.ShapeDtypeStruct(shape, dtype) for shape, dtype in outs],
        in_specs=specs,
        out_specs=[VMEM] * len(outs),
        scratch_shapes=list(scratch),
        compiler_params=params,
        cost_estimate=pl.CostEstimate(flops=flops, bytes_accessed=bytes_accessed, transcendentals=0),
    )(*args)


def exchange(values, axis, size, mask):
    return lax.ppermute(values, axis, [(at, at ^ mask) for at in range(size)])


def stream_rows(design_ref, buffers, sems, row_of, steps, tile, use):
    depth = buffers.shape[0]

    def copy(step):
        slot = lax.rem(step, depth)
        return pltpu.make_async_copy(
            design_ref.at[pl.ds(pl.multiple_of(row_of(step), tile), tile), :], buffers.at[slot], sems.at[slot]
        )

    def begin():
        for step in range(min(depth, steps)):
            copy(step).start()

    def run():
        def one(step, carry):
            copy(step).wait()
            use(step, buffers[lax.rem(step, depth)])

            @pl.when(step + depth < steps)
            def _():
                copy(step + depth).start()

            return carry

        lax.fori_loop(0, steps, one, 0)

    return begin, run


def place_shares(where, stacks, target, samples, rhs, width):
    for across in range(rhs):
        for mask in range(samples):
            share = (where[2] ^ across) * samples + (where[1] ^ mask)
            target[:, pl.ds(pl.multiple_of(share * width, width), width)] = stacks[across][mask]


def times_columns(block, left):
    pieces = 4
    width = left.shape[1] // pieces
    cut = width * 3 // 4 if width * 3 % 1024 == 0 else width // 2
    streamed, held = None, None
    for start in range(0, pieces * width, width):
        one = lax.dot_general(block[:, start : start + cut], left[:, start : start + cut], NT, preferred_element_type=f32)
        span = slice(start + cut, start + width)
        two = lax.dot_general(left[:, span], block[:, span], NT, preferred_element_type=f32)
        streamed = one if streamed is None else streamed + one
        held = two if held is None else held + two
    return jnp.swapaxes(streamed, 0, 1) + held


def forward_pass(where, stacks, design, masks, sizes):
    samples, feats, rhs = sizes
    rows, depth = design.shape
    cols = stacks[0].shape[1]
    chunk = rows // feats
    tile = min(256, chunk)
    per = chunk // tile
    width = depth // (samples * rhs)

    def body(where_ref, design_ref, *refs):
        stack_refs = refs[:rhs]
        outs = refs[rhs : rhs + len(masks)]
        buffers, joined, sems = refs[rhs + len(masks) :]
        at = [where_ref[i] for i in range(3)]

        def row_of(step):
            return (at[0] ^ (masks[0] - step // per)) * chunk + lax.rem(step, per) * tile

        def use(step, block):
            out = times_columns(block, joined[...]).astype(bf16)
            start = pl.multiple_of(lax.rem(step, per) * tile, tile)
            for group in range(len(masks)):

                @pl.when(step // per == group)
                def _(group=group):
                    outs[group][:, pl.ds(start, tile)] = out

        begin, run = stream_rows(design_ref, buffers, sems, row_of, len(masks) * per, tile, use)
        begin()
        place_shares(at, stack_refs, joined, samples, rhs, width)
        run()

    work = len(masks) * chunk * depth
    return call(
        body,
        [((cols, chunk), bf16)] * len(masks),
        (where, design, *stacks),
        [SMEM, HBM] + [VMEM] * rhs,
        scratch=(
            pltpu.VMEM((4, tile, depth), bf16),
            pltpu.VMEM((cols, depth), bf16),
            pltpu.SemaphoreType.DMA((4,)),
        ),
        flops=2 * work * cols,
        bytes_accessed=2 * work,
        limit=40 << 20,
    )


def backward_pass(where, pieces, design, masks, sizes, carried=None):
    samples, feats, rhs = sizes
    rows, depth = design.shape
    cols = pieces[0].shape[0]
    chunk = rows // feats
    tile = min(128, chunk)
    per = chunk // tile
    width = depth // (samples * rhs)
    n = len(masks)

    def body(where_ref, design_ref, *refs):
        piece_refs = refs[:n]
        last = carried is not None
        if last:
            start_ref, mine_ref, theirs_ref, buffers, joined, sems, total = refs[n:]
        else:
            total, buffers, joined, sems = refs[n:]
        at = [where_ref[i] for i in range(3)]

        def row_of(step):
            return (at[0] ^ (masks[0] + step // per)) * chunk + lax.rem(step, per) * tile

        def use(step, block):
            left = joined[:, pl.ds(pl.multiple_of(step * tile, tile), tile)]
            total[...] += jnp.dot(left, block, preferred_element_type=f32)

        begin, run = stream_rows(design_ref, buffers, sems, row_of, n * per, tile, use)
        begin()
        for group in range(n):
            joined[:, group * chunk : (group + 1) * chunk] = piece_refs[group][...]
        total[...] = start_ref[...] if last else jnp.zeros_like(total)
        run()
        if last:
            for side, out in ((0, mine_ref), (1, theirs_ref)):
                for mask in range(samples):
                    share = (at[2] ^ side) * samples + (at[1] ^ mask)
                    out[mask] = total[:, pl.ds(pl.multiple_of(share * width, width), width)].astype(bf16)

    work = n * chunk * depth
    buffers = pltpu.VMEM((8, tile, depth), bf16)
    sems = (pltpu.VMEM((cols, n * chunk), bf16), pltpu.SemaphoreType.DMA((8,)))
    args = (where, design, *pieces)
    specs = [SMEM, HBM] + [VMEM] * n
    if carried is None:
        outs = [((cols, depth), f32)]
        scratch = (buffers, *sems)
    else:
        outs = [((samples, cols, width), bf16)] * 2
        args += (carried,)
        specs += [VMEM]
        scratch = (buffers, *sems, pltpu.VMEM((cols, depth), f32))
    return call(
        body, outs, args, specs, scratch=scratch, flops=2 * work * cols, bytes_accessed=2 * work, limit=40 << 20
    )


def merge(mine, theirs, samples, rhs, sent_dtype):
    came = exchange(theirs, "rhs", rhs, 1)
    sums = [mine[mask].astype(f32) + came[mask].astype(f32) for mask in range(samples)]
    return [sums[0]] + [one.astype(sent_dtype) for one in sums[1:]]


def sum_small(values, sizes):
    for axis, size in zip(("samples", "features", "rhs"), sizes):
        came = [exchange(values, axis, size, mask) for mask in range(1, size)]
        for one in came:
            values = values + one
    return values


def sum_features(total, size):
    whole = total
    for mask in range(1, size):
        whole = whole + exchange(total, "features", size, mask)
    return whole


def share_all(values, samples, rhs):
    stack = jnp.stack([values] + [exchange(values, "samples", samples, mask) for mask in range(1, samples)])
    return [stack] + [exchange(stack, "rhs", rhs, mask) for mask in range(1, rhs)]


def sum_all(mine, theirs, sizes):
    samples, feats, rhs = sizes
    pieces = merge(mine, theirs, samples, rhs, f32)
    total = pieces[0]
    for mask in range(1, samples):
        total = total + exchange(pieces[mask], "samples", samples, mask)
    return share_all(sum_features(total, feats), samples, rhs)


def write_halves(where_ref, packed, mine_ref, theirs_ref):
    samples, _, width = mine_ref.shape
    for side, out in ((0, mine_ref), (1, theirs_ref)):
        for mask in range(samples):
            share = (where_ref[2] ^ side) * samples + (where_ref[1] ^ mask)
            out[mask] = packed[:, pl.ds(pl.multiple_of(share * width, width), width)]


def first_products(where, near, far, factor, width):
    part, depth = near.shape
    last_start = factor.shape[1] - width

    def body(where_ref, near_ref, far_ref, factor_ref, out_ref, share_ref, sem):
        start = pl.multiple_of(jnp.minimum(where_ref[1] * width, last_start), width)
        copy = pltpu.make_async_copy(factor_ref.at[:, pl.ds(start, width)], share_ref, sem)
        copy.start()
        copy.wait()
        both = jnp.concatenate([near_ref[...], far_ref[...]])
        found = with_narrow(both, share_ref[...], (((1,), (0,)), ((), ())))
        for side in range(2):
            out_ref[pl.ds(pl.multiple_of((where_ref[2] ^ side) * part, part), part), :] = found[side * part : (side + 1) * part]

    return call(
        body,
        [((2 * part, width), f32)],
        (where, near, far, factor),
        [SMEM, VMEM, VMEM, HBM],
        scratch=(pltpu.VMEM((depth, width), bf16), pltpu.SemaphoreType.DMA),
    )[0]


def first_update(where, stacks, res, basis, shrink, sizes):
    samples, _, rhs = sizes
    cols, own = res.shape
    rank = basis.shape[1]
    width = stacks[0].shape[2]
    wide = width * samples * rhs

    def body(where_ref, *refs):
        stack_refs = refs[:rhs]
        res_ref, basis_ref, shrink_ref, proj_ref, dir_ref, narrow_ref, packed = refs[rhs:]
        at = [where_ref[i] for i in range(3)]
        place_shares(at, stack_refs, packed, samples, rhs, width)
        side = wide // rhs
        for across in range(rhs):
            proj_ref[:, across * (rank // rhs) : (across + 1) * (rank // rhs)] = packed[:, across * side : across * side + rank // rhs]
        proj = proj_ref[...]
        direction = res_ref[...] + with_narrow(proj * shrink_ref[...], basis_ref[...], NT)
        dir_ref[...] = direction
        narrow_ref[...] = direction.astype(bf16)

    return call(
        body,
        [((cols, rank), f32), ((cols, own), f32), ((cols, own), bf16)],
        (where, *stacks, res, basis, shrink),
        [SMEM] + [VMEM] * (rhs + 3),
        scratch=(pltpu.VMEM((cols, wide), f32),),
    )


def products(where, kept, arrived, direction, res, basis, wide, sizes):
    cols, own = res.shape
    rank = basis.shape[1]
    n = len(arrived)

    def body(where_ref, kept_ref, *refs):
        arrived_refs = refs[:n]
        dir_ref, res_ref, basis_ref, applied_ref, mine_ref, theirs_ref, packed = refs[n:]
        applied = kept_ref[...]
        for ref in arrived_refs:
            applied = applied + ref[...].astype(f32)
        direction_now, residual = dir_ref[...], res_ref[...]
        applied = applied + ridge_weight * direction_now
        applied_ref[...] = applied
        packed[...] = jnp.zeros_like(packed)
        found = exact(jnp.concatenate([direction_now, applied, residual]), applied, NT)
        packed[:, rank : rank + cols] = found[:cols]
        packed[:, rank + cols : rank + 2 * cols] = exact(residual, direction_now, NT)
        packed[:, :rank] = with_narrow(applied, basis_ref[...], (((1,), (0,)), ((), ())))
        packed[:, rank + 2 * cols : rank + 3 * cols] = found[cols : 2 * cols]
        packed[:, rank + 3 * cols : rank + 4 * cols] = found[2 * cols :]
        write_halves(where_ref, packed, mine_ref, theirs_ref)

    return call(
        body,
        [((cols, own), f32)] + [((sizes[0], cols, wide // (sizes[0] * sizes[2])), f32)] * 2,
        (where, kept, *arrived, direction, res, basis),
        [SMEM] + [VMEM] * (n + 4),
        scratch=(pltpu.VMEM((cols, wide), f32),),
    )


def inverse(matrix):
    size = matrix.shape[0]
    row_at = lax.broadcasted_iota(jnp.int32, (size, 1), 0)
    unit = lax.broadcasted_iota(jnp.int32, (size, size), 0) == lax.broadcasted_iota(jnp.int32, (size, size), 1)
    work = jnp.concatenate([matrix, unit.astype(f32)], axis=1)
    for k in range(size):
        recip = 1.0 / work[k : k + 1, k : k + 1]
        row = work[k : k + 1, :] * recip
        work = jnp.where(row_at == k, row, work - work[:, k : k + 1] * row)
    return work[:, size:]


def update(where, stacks, proj, direction, applied, res, basis, shrink, sizes):
    samples, _, rhs = sizes
    cols, own = res.shape
    rank = basis.shape[1]
    width = stacks[0].shape[2]
    wide = width * samples * rhs

    def body(where_ref, *refs):
        stack_refs = refs[:rhs]
        proj_ref, dir_ref, applied_ref, res_ref, basis_ref, shrink_ref, step_ref, new_res_ref = refs[rhs : rhs + 8]
        packed = refs[-1]
        at = [where_ref[i] for i in range(3)]
        place_shares(at, stack_refs, packed, samples, rhs, width)
        gram = packed[:, rank : rank + cols]
        gram = 0.5 * (gram + jnp.swapaxes(gram, 0, 1))
        inv = inverse(gram)
        inv = 0.5 * (inv + jnp.swapaxes(inv, 0, 1))
        step = exact(packed[:, rank + cols : rank + 2 * cols], inv)
        step_ref[...] = step
        residual = res_ref[...] - exact(step, applied_ref[...])
        new_res_ref[...] = residual
        new_proj_ref, new_dir_ref, narrow_ref = refs[rhs + 8 : -1]
        image = packed[:, :rank]
        new_proj = proj_ref[...] - exact(step, image)
        new_proj_ref[...] = new_proj
        scaled = new_proj * shrink_ref[...]
        cross = packed[:, rank + 3 * cols : rank + 4 * cols] - exact(step, packed[:, rank + 2 * cols : rank + 3 * cols])
        cross = cross + exact(scaled, image, NT)
        next_coef = -exact(cross, inv)
        new_dir = residual + with_narrow(scaled, basis_ref[...], NT) + exact(next_coef, dir_ref[...])
        new_dir_ref[...] = new_dir
        narrow_ref[...] = new_dir.astype(bf16)

    outs = [((cols, cols), f32), ((cols, own), f32)]
    outs += [((cols, rank), f32), ((cols, own), f32), ((cols, own), bf16)]
    return call(
        body,
        outs,
        (where, *stacks, proj, direction, applied, res, basis, shrink),
        [SMEM] + [VMEM] * (rhs + 6),
        scratch=(pltpu.VMEM((cols, wide), f32),),
    )


def gram_part(kept, came, direction, res):
    cols, chunk = kept.shape
    n = len(came)

    def body(kept_ref, *refs):
        dir_ref, res_ref, image_ref, gram_ref = refs[n:]
        total = kept_ref[...].astype(f32)
        for ref in refs[:n]:
            total = total + ref[...].astype(f32)
        image = total.astype(bf16)
        image_ref[...] = image
        direction_now = dir_ref[...]
        gram = exact(total, image.astype(f32), NT) + ridge_weight * exact(direction_now, direction_now, NT)
        gram_ref[:, :cols] = gram
        gram_ref[:, cols:] = exact(res_ref[...], direction_now, NT)

    return call(body, [((cols, chunk), bf16), ((cols, 2 * cols), f32)], (kept, *came, direction, res), [VMEM] * (n + 3))


def last_step(grams):
    cols = grams.shape[0]

    def body(gram_ref, step_ref):
        gram = gram_ref[:, :cols]
        inv = inverse(0.5 * (gram + jnp.swapaxes(gram, 0, 1)))
        step_ref[...] = exact(gram_ref[:, cols:], 0.5 * (inv + jnp.swapaxes(inv, 0, 1)))

    return call(body, [((cols, cols), f32)], (grams,), [VMEM], flops=10**9)[0]


def last_residual(where, kept, arrived, direction, res, step, part):
    cols, own = res.shape
    n = len(arrived)

    def body(where_ref, kept_ref, *refs):
        dir_ref, res_ref, step_ref, same_ref, other_ref, whole = refs[n:]
        applied = kept_ref[...]
        for ref in refs[:n]:
            applied = applied + ref[...].astype(f32)
        applied = applied + ridge_weight * dir_ref[...]
        whole[...] = res_ref[...] - exact(step_ref[...], applied)
        same_ref[...] = whole[pl.ds(pl.multiple_of(where_ref[2] * part, part), part), :].astype(bf16)
        other_ref[...] = whole[pl.ds(pl.multiple_of((where_ref[2] ^ 1) * part, part), part), :].astype(bf16)

    return call(
        body,
        [((part, own), bf16)] * 2,
        (where, kept, *arrived, direction, res, step),
        [SMEM] + [VMEM] * (n + 4),
        scratch=(pltpu.VMEM((cols, own), f32),),
    )


def collect(where, all_stacks, steps, sizes):
    samples, _, rhs = sizes
    cols, width = all_stacks[0][0].shape[1:]
    part = cols // rhs
    count = len(all_stacks)
    depth = width * samples * rhs

    def body(where_ref, *refs):
        stack_refs, step_refs, out_ref = refs[: count * rhs], refs[count * rhs : -1], refs[-1]
        at = [where_ref[i] for i in range(3)]
        rows = pl.ds(pl.multiple_of(at[2] * part, part), part)
        coefs = [ref[rows, :] for ref in step_refs]
        for across in range(rhs):
            for mask in range(samples):
                share = (at[2] ^ across) * samples + (at[1] ^ mask)
                total = jnp.zeros((part, width), f32)
                for k in range(count):
                    upper = coefs[k].astype(bf16)
                    lower = (coefs[k] - upper.astype(f32)).astype(bf16)
                    block = stack_refs[k * rhs + across][mask]
                    total += jnp.dot(upper, block, preferred_element_type=f32)
                    total += jnp.dot(lower, block, preferred_element_type=f32)
                out_ref[:, pl.ds(pl.multiple_of(share * width, width), width)] = total

    return call(
        body,
        [((part, depth), f32)],
        (where, *[one for stacks in all_stacks for one in stacks], *steps),
        [SMEM] + [VMEM] * (count * rhs + count),
    )[0]


def shards(sizes, design, right_side, factor, nystrom_values):
    samples, feats, rhs = sizes
    depth, col_share = right_side.shape
    own = depth // (samples * rhs)
    at_sample, at_feat, at_rhs = lax.axis_index("samples"), lax.axis_index("features"), lax.axis_index("rhs")
    where = jnp.stack([at_feat, at_sample, at_rhs]).astype(jnp.int32)
    shrink = ((1.0 + jnp.min(nystrom_values)) / (1.0 + nystrom_values) - 1.0)[None, :]
    rank = shrink.shape[1]
    cols = col_share * rhs
    unit = 128 * samples * rhs
    wide = -(-(rank + 4 * cols) // unit) * unit

    share = at_rhs * samples + at_sample
    other_share = (1 - at_rhs) * samples + at_sample
    near = right_side.T
    far = exchange(near, "rhs", rhs, 1)
    found = sum_features(first_products(where, near, far, factor, wide // (samples * rhs)), feats)
    proj_stacks = share_all(found, samples, rhs)
    own_near = lax.dynamic_slice_in_dim(near, share * own, own, 1)
    own_far = lax.dynamic_slice_in_dim(far, share * own, own, 1)
    res = jnp.where(at_rhs == 0, jnp.concatenate([own_near, own_far]), jnp.concatenate([own_far, own_near]))
    mine = lax.dynamic_slice_in_dim(factor, share * own, own, 0)
    came = exchange(lax.dynamic_slice_in_dim(factor, other_share * own, own, 0), "rhs", rhs, 1)
    basis = jnp.where(at_rhs == 0, jnp.concatenate([mine, came], 1), jnp.concatenate([came, mine], 1))
    proj, direction, narrow = first_update(where, proj_stacks, res, basis, shrink, sizes)
    all_stacks, steps = [], []
    for iteration in range(ITERS):
        last = iteration + 1 == ITERS
        stacks = share_all(narrow, samples, rhs)
        all_stacks.append(stacks)
        away = list(range(feats - 1, 0, -1))
        sent = forward_pass(where, stacks, design, away, sizes)
        came = [exchange(value, "features", feats, mask) for value, mask in zip(sent, away)]
        (kept,) = forward_pass(where, stacks, design, [0], sizes)
        if last:
            image, grams = gram_part(kept, came, direction, res)
            grams = sum_small(grams, sizes)
        else:
            total = kept.astype(f32)
            for value in came:
                total = total + value.astype(f32)
            image = total.astype(bf16)
        others = [exchange(image, "features", feats, mask) for mask in range(1, feats)]
        (carried,) = backward_pass(where, [image], design, [0], sizes)
        mine, theirs = backward_pass(where, others, design, list(range(1, feats)), sizes, carried)
        pieces = merge(mine, theirs, samples, rhs, bf16)
        arrived = [exchange(pieces[mask], "samples", samples, mask) for mask in range(1, samples)]
        if last:
            step = last_step(grams)
            same, other = last_residual(where, pieces[0], arrived, direction, res, step, col_share)
        else:
            applied, *halves = products(where, pieces[0], arrived, direction, res, basis, wide, sizes)
            sums = sum_all(*halves, sizes)
            step, res, proj, direction, narrow = update(
                where, sums, proj, direction, applied, res, basis, shrink, sizes
            )
        steps.append(step)
    pair = jnp.stack([same, exchange(other, "rhs", rhs, 1)])
    parts = jnp.stack([pair] + [exchange(pair, "samples", samples, mask) for mask in range(1, samples)])
    out_sol = collect(where, all_stacks, steps, sizes).T
    order = jnp.arange(samples) ^ at_sample
    sides = jnp.arange(rhs) ^ at_rhs
    parts = parts[order][:, sides]
    out_res = parts.transpose(1, 0, 3, 2).reshape(depth, col_share).astype(f32)
    return (out_sol, out_res)


def solution(mesh):
    sizes = (mesh.shape["samples"], mesh.shape["features"], mesh.shape["rhs"])
    placed = (P(("samples", "rhs"), "features"), P("features", "rhs"), P("features", "rhs"), P())
    return jax.shard_map(
        functools.partial(shards, sizes),
        mesh=mesh,
        in_specs=placed,
        out_specs=(P("features", "rhs"), P("features", "rhs")),
        check_vma=False,
    )
```
